128 devices in a mesh: dp: 64 (over z, y, x), mp: 2 (over core).
Axes of the slice: x: 4, y: 4, z: 4, core: 2. Of those that a mesh axis runs over, the one named last changes fastest.
Arguments:
- pixels: bfloat16 [128, 512, 768], P(('dp', 'mp')), may hold values from -6 to 6
- counts: int32 [64, 2], P('dp'), may hold values from 128 to 512
- owner: int32 [64, 2], P('dp'), may hold values from 0 to 1, each once within a row
- embed_weight: bfloat16 [768, 1024], P('dp', 'mp'), may hold values from -0.21875 to 0.21875
- w_qkv: bfloat16 [3, 1024, 1024], P(None, 'dp', 'mp'), may hold values from -0.8 to 0.8
- w_out: bfloat16 [1024, 1024], P('mp', 'dp'), may hold values from -0.1875 to 0.1875
- w_up: bfloat16 [1024, 4096], P('dp', 'mp'), may hold values from -0.1875 to 0.1875
- w_down: bfloat16 [4096, 1024], P('mp', 'dp'), may hold values from -0.09375 to 0.09375
- ln1_gain: float32 [1024], replicated, may hold values from 0.25 to 1.75
- ln2_gain: float32 [1024], replicated, may hold values from 0.25 to 1.75
- targets: bfloat16 [64, 2, 512, 1024], P('dp', None, 'mp'), may hold values from -20 to 20
Outputs:
- encoded: bfloat16 [64, 2, 512, 1024], P('dp', None, 'mp')
- mean_loss: float32 [], replicated
The draws below stay inside these ranges and needn't reach their ends.
Inputs may be any that keep to these rules, and one draw needn't show every extreme that they name: counts[g, r] is the number of valid patches at the start of image g * 2 + r; the remaining patch slots are padding. Each row owner[g, :] is a permutation of 0 to 2 - 1, so every held image is encoded once.
All inputs are finite; a program needn't handle non-finite values.
Results may differ from the reference program's by a relative error of at most 0.014.
Values may be sent and summed in bfloat16 or wider, within the bound.
A program may use at most 128 MiB of HBM per device.

```python
import math
import jax
import jax.numpy as jnp
from jax import lax

D = 1024
HEADS = 16
HEAD = 64
FF = 4096
PIX = 768
PATCHES = 512
IMAGES = 128
N_DP = 64
N_MP = 2


def draw_w_qkv(key, part):
    base = jax.random.normal(jax.random.fold_in(key, 11), (3, D, D), jnp.float32)
    stacked = base / math.sqrt(D)
    return jnp.clip(stacked, -0.78, 0.78).astype(jnp.bfloat16)


def draw_targets(key, part):
    place = jnp.arange(N_DP, dtype=jnp.float32) / max(N_DP - 1, 1)
    values = jax.random.normal(jax.random.fold_in(key, 22), (N_DP, N_MP, PATCHES, D), jnp.float32)
    scale = 0.5 + 2.0 * place
    return jnp.clip(values * scale[:, None, None, None], -20.0, 20.0).astype(jnp.bfloat16)


def place_ends(values, own_key, smallest, top_value):
    spot = [jax.random.randint(jax.random.fold_in(own_key, axis), (), 0, length) for axis, length in enumerate(values.shape)]
    longest = values.shape.index(max(values.shape))
    next_to = spot[:longest] + [(spot[longest] + 1) % values.shape[longest]] + spot[longest + 1:]
    return values.at[tuple(spot)].set(smallest).at[tuple(next_to)].set(top_value)


def steps_of(stream_key, extent, shards, smallest, high):
    def one(dim, shards_of):
        steps = jax.random.uniform(jax.random.fold_in(jax.random.fold_in(stream_key, 6), dim), (shards_of,), jnp.float32, smallest / len(shards), high / len(shards))
        return jnp.repeat(jnp.exp(steps), extent[dim] // shards_of).reshape((-1,) + (1,) * (len(extent) - dim - 1))

    gain = one(*shards[0])
    for cut in shards[1:]:
        gain = gain * one(*cut)
    return gain


def scatter_about(own_key, shape, deviation, bound, pieces=(), kind=jnp.bfloat16):
    result = jax.random.normal(own_key, shape, jnp.float32) * deviation
    if len(pieces) > 0:
        result = steps_of(own_key, shape, pieces, -0.22, 0.18) * result
    return jnp.clip(result, min=-bound, max=bound).astype(kind)


def setup_inputs(seed: int = 0) -> dict:
    splits = jax.random.split(jax.random.key(seed), 12)
    return {
        "pixels": scatter_about(splits[0], (IMAGES, PATCHES, PIX), 1.0, 6.0, ((0, 128),)),
        "counts": place_ends(jax.random.randint(splits[1], (N_DP, N_MP), PATCHES // 4, PATCHES + 1), jax.random.fold_in(splits[1], 1), PATCHES // 4, PATCHES).astype(jnp.int32),
        "owner": jax.vmap(lambda own: jax.random.permutation(own, N_MP))(jax.random.split(splits[2], N_DP)).reshape((N_DP, N_MP)).astype(jnp.int32),
        "embed_weight": scatter_about(splits[3], (PIX, D), PIX ** -0.5, 0.21875, ((0, 64), (1, 2))),
        "w_qkv": draw_w_qkv(jax.random.fold_in(splits[11], 71), 0),
        "w_out": scatter_about(splits[5], (D, D), D ** -0.5, 0.1875, ((0, 2), (1, 64))),
        "w_up": scatter_about(splits[6], (D, FF), D ** -0.5, 0.1875, ((0, 64), (1, 2))),
        "w_down": scatter_about(splits[7], (FF, D), FF ** -0.5, 0.09375, ((0, 2), (1, 64))),
        "ln1_gain": jnp.clip(1.0 + 0.15 * jax.random.normal(splits[8], (D,), jnp.float32), 0.25, 1.75),
        "ln2_gain": jnp.clip(1.0 + 0.15 * jax.random.normal(splits[9], (D,), jnp.float32), 0.25, 1.75),
        "targets": draw_targets(jax.random.fold_in(splits[11], 71), 0),
    }


def layer_norm(inputs, gains):
    average = lax.optimization_barrier(jnp.mean(inputs, axis=-1, keepdims=True))
    centred = inputs - average
    spread = lax.optimization_barrier(jnp.mean(centred * centred, axis=-1, keepdims=True))
    return centred * lax.rsqrt(spread + 1e-06) * gains.astype(jnp.float32)

def group_sum(left_mat, right_mat, groups):
    row_count = left_mat.shape[0]
    column_width = left_mat.shape[1] // groups
    left_part = left_mat.reshape(row_count, groups, column_width).astype(jnp.float32)
    right_part = right_mat.reshape(groups, column_width, right_mat.shape[1]).astype(jnp.float32)
    partial_value = jnp.einsum('pgh,ghd->gpd', left_part, right_part).astype(jnp.bfloat16)
    partial_value = lax.optimization_barrier(partial_value)
    return lax.optimization_barrier(jnp.sum(partial_value.astype(jnp.float32), axis=0))

def encode_image(picture, length, wanted, embed_weight, w_qkv, w_out, w_up, w_down, ln1_gain, ln2_gain):
    tokens = jnp.dot(picture, embed_weight, preferred_element_type=jnp.float32).astype(jnp.bfloat16)
    normed = layer_norm(tokens.astype(jnp.float32), ln1_gain).astype(jnp.bfloat16)
    factor = HEAD ** (-0.5)
    queries = (jnp.dot(normed, w_qkv[0], preferred_element_type=jnp.float32) * factor).astype(jnp.bfloat16)
    key_rows = jnp.dot(normed, w_qkv[1], preferred_element_type=jnp.float32).astype(jnp.bfloat16)
    value_rows = jnp.dot(normed, w_qkv[2], preferred_element_type=jnp.float32).astype(jnp.bfloat16)
    queries = queries.reshape(PATCHES, HEADS, HEAD)
    key_rows = key_rows.reshape(PATCHES, HEADS, HEAD)
    value_rows = value_rows.reshape(PATCHES, HEADS, HEAD)
    scores = jnp.einsum('qhd,khd->hqk', queries.astype(jnp.float32), key_rows.astype(jnp.float32))
    usable = jnp.arange(PATCHES, dtype=jnp.int32) < length
    scores = jnp.where(usable[None, None, :], scores, -1e+30)
    row_max = lax.optimization_barrier(jnp.max(scores, axis=-1, keepdims=True))
    expo = jnp.exp(scores - row_max)
    row_sum = lax.optimization_barrier(jnp.sum(expo, axis=-1))
    probs = lax.optimization_barrier(expo.astype(jnp.bfloat16))
    mixture = jnp.einsum('hqk,khd->qhd', probs.astype(jnp.float32), value_rows.astype(jnp.float32))
    mixture = mixture / jnp.transpose(row_sum)[:, :, None]
    attended = mixture.astype(jnp.bfloat16).reshape(PATCHES, D)
    residual = tokens.astype(jnp.float32) + group_sum(attended, w_out, N_MP)
    normed_two = layer_norm(residual, ln2_gain).astype(jnp.bfloat16)
    hidden = jax.nn.gelu(jnp.dot(normed_two, w_up, preferred_element_type=jnp.float32), approximate=False).astype(jnp.bfloat16)
    output = residual + group_sum(hidden, w_down, N_MP)
    misfit = output - wanted.astype(jnp.float32)
    squares = jnp.sum(jnp.where(usable[:, None], misfit * misfit, 0.0))
    number = jnp.sum(usable.astype(jnp.float32))
    return (output.astype(jnp.bfloat16), squares, number)

def reference(pixels, counts, owner, embed_weight, w_qkv, w_out, w_up, w_down, ln1_gain, ln2_gain, targets):
    order = owner.astype(jnp.int32)
    image_ids = (jnp.arange(N_DP, dtype=jnp.int32)[:, None] * N_MP + order).reshape(-1)
    lengths = jnp.take_along_axis(counts.astype(jnp.int32), order, axis=1).reshape(-1)
    wanted_all = targets.reshape(N_DP * N_MP, PATCHES, D)

    def encode_group(inputs):
        index, length, wanted = inputs
        picture = lax.dynamic_index_in_dim(pixels, index, 0, keepdims=False)
        return encode_image(picture, length, wanted, embed_weight, w_qkv, w_out, w_up, w_down, ln1_gain, ln2_gain)
    encoded, squares, number = lax.map(encode_group, (image_ids, lengths, wanted_all))
    mean_loss = jnp.sum(squares) / (D * jnp.sum(number))
    return (encoded.reshape(N_DP, N_MP, PATCHES, D), mean_loss)
```

```python
import jax
import jax.numpy as jnp
from jax import lax
from jax.experimental import pallas as pl
from jax.experimental.pallas import tpu as pltpu
from jax.sharding import Mesh
from jax.sharding import PartitionSpec as P

D = 1024
HEAD = 64
DP = ("dp_0", "dp_1", "dp_2")
DP_MP = ("dp_0", "dp_1", "dp_2", "mp")
MESH = pl.DeviceIdType.MESH
TILE = 128
ORDERS = ((2, 1, 0), (1, 0, 2), (0, 2, 1))
BATCHES = ((6, 5, 5), (4, 4, 4), (4, 4, 4), (4, 4, 4))
UP_TILES = (4, 6, 6)
COLUMNS = TILE * sum(sum(b) for b in BATCHES)


def spans():
    out, at = [], 0
    for batch in BATCHES:
        row = []
        for tiles in batch:
            row.append((at * TILE, tiles * TILE))
            at += tiles
        out.append(row)
    return out


SPANS = spans()


class Gather:

    def __init__(self, own_ref, whole_ref, send_sems, recv_sems):
        self.own, self.whole = own_ref, whole_ref
        self.send, self.recv = send_sems, recv_sems
        self.me = [lax.axis_index(a) for a in DP]
        self.half = lax.axis_index("mp")
        self.copies = {}
        self.count = 0
        self.started = []

    def region(self, order, phase, coord, start, size):
        at = [None, None, None]
        for i in range(3):
            axis = order[i]
            at[axis] = pl.ds(0, 4) if i < phase else (coord if i == phase else self.me[axis])
        return self.whole.at[self.half, at[0], at[1], at[2], :, pl.ds(start, size)]

    def copy(self, key, src, dst, device):
        made = pltpu.make_async_remote_copy(
            src_ref=src,
            dst_ref=dst,
            send_sem=self.send.at[self.count],
            recv_sem=self.recv.at[self.count],
            device_id=device,
            device_id_type=MESH,
        )
        self.count += 1
        made.start()
        self.started.append(made)
        self.copies[key] = made

    def ring(self, batch, colour, phase):
        order = ORDERS[colour]
        axis = order[phase]
        mine = self.me[axis]
        right, left = lax.rem(mine + 1, 4), lax.rem(mine + 3, 4)
        return order, DP[axis], mine, right, left

    def step_a(self, batch, phase):
        for colour in range(3):
            if phase > 0:
                for side in "rl":
                    self.copies[batch, colour, phase - 1, "b", side].wait_recv()
            order, name, mine, right, left = self.ring(batch, colour, phase)
            start, size = SPANS[batch][colour]
            block = self.region(order, phase, mine, start, size)
            src = block if phase else self.own.at[:, pl.ds(start, size)]
            self.copy((batch, colour, phase, "a", "r"), src, block, {name: right})
            self.copy((batch, colour, phase, "a", "l"), src, block, {name: left})
            if phase == 2:
                self.across(batch, colour, mine)

    def step_b(self, batch, phase):
        for colour in range(3):
            for side in "rl":
                self.copies[batch, colour, phase, "a", side].wait_recv()
            order, name, mine, right, left = self.ring(batch, colour, phase)
            start, size = SPANS[batch][colour]
            first = size // TILE // 2 * TILE
            from_left = self.region(order, phase, left, start, first)
            from_right = self.region(order, phase, right, start + first, size - first)
            self.copy((batch, colour, phase, "b", "r"), from_left, from_left, {name: right})
            self.copy((batch, colour, phase, "b", "l"), from_right, from_right, {name: left})
            if phase == 2:
                self.across(batch, colour, left)
                self.across(batch, colour, right)

    def across(self, batch, colour, coord):
        start, size = SPANS[batch][colour]
        block = self.region(ORDERS[colour], 2, coord, start, size)
        kind = sum(1 for k in self.copies if k[:2] == (batch, colour) and k[2] == "x")
        self.copy((batch, colour, "x", kind), block, block, {"mp": 1 - self.half})

    def finish(self, batch):
        for colour in range(3):
            for side in "rl":
                self.copies[batch, colour, 2, "b", side].wait_recv()
            mine = self.me[ORDERS[colour][2]]
            self.across(batch, colour, lax.rem(mine + 2, 4))

    def arrived(self, batch):
        for colour in range(3):
            for kind in range(4):
                self.copies[batch, colour, "x", kind].wait_recv()

    def drain(self):
        for made in self.started:
            made.wait_send()


def greet():
    barrier = pltpu.get_barrier_semaphore()
    count = 0
    for name in DP:
        mine = lax.axis_index(name)
        for step in (1, 3):
            pl.semaphore_signal(
                barrier, inc=1, device_id={name: lax.rem(mine + step, 4)}, device_id_type=MESH
            )
            count += 1
    pl.semaphore_signal(
        barrier, inc=1, device_id={"mp": 1 - lax.axis_index("mp")}, device_id_type=MESH
    )
    pl.semaphore_wait(barrier, count + 1)


N_COPIES = len(BATCHES) * 3 * 16


def gather_kernel(own_ref, whole_ref, send_sems, recv_sems, local_sem):
    greet()
    g = Gather(own_ref, whole_ref, send_sems, recv_sems)
    here = pltpu.make_async_copy(
        own_ref, whole_ref.at[g.half, g.me[0], g.me[1], g.me[2]], local_sem
    )
    here.start()
    for b in range(4):
        g.step_a(b, 0)
    for b in range(4):
        g.step_b(b, 0)
    here.wait()
    g.step_a(0, 1)
    g.step_a(1, 1)
    g.step_b(0, 1)
    g.step_a(0, 2)
    g.step_b(1, 1)
    g.step_a(2, 1)
    g.step_b(0, 2)
    g.step_b(2, 1)
    g.step_a(1, 2)
    g.step_a(3, 1)
    g.finish(0)
    g.step_b(1, 2)
    g.step_b(3, 1)
    g.step_a(2, 2)
    g.finish(1)
    g.step_b(2, 2)
    g.step_a(3, 2)
    g.finish(2)
    g.step_b(3, 2)
    g.finish(3)
    for b in range(4):
        g.arrived(b)
    g.drain()


def gather_weights(line):
    return pl.pallas_call(
        gather_kernel,
        out_shape=jax.ShapeDtypeStruct((2, 4, 4, 4, 16, COLUMNS), jnp.bfloat16),
        in_specs=[pl.BlockSpec(memory_space=pltpu.VMEM)],
        out_specs=pl.BlockSpec(memory_space=pltpu.VMEM),
        scratch_shapes=[
            pltpu.SemaphoreType.DMA((N_COPIES,)),
            pltpu.SemaphoreType.DMA((N_COPIES,)),
            pltpu.SemaphoreType.DMA,
        ],
        compiler_params=pltpu.CompilerParams(
            collective_id=0, has_side_effects=True, vmem_limit_bytes=64 * 1024 * 1024 - 65536
        ),
        name="gather_weights",
    )(line)


def layer_norm(inputs, gains):
    average = jnp.mean(inputs, axis=-1, keepdims=True)
    centred = inputs - average
    spread = jnp.mean(centred * centred, axis=-1, keepdims=True)
    return centred * lax.rsqrt(spread + 1e-06) * gains


def on_device(
    pixels, counts, owner, embed_weight, w_qkv, w_out, w_up, w_down, ln1_gain, ln2_gain, targets
):
    picture = pixels[0]
    patches = picture.shape[0]
    me = lax.axis_index("mp")
    embed = jnp.pad(embed_weight, ((0, 4), (0, 0)))
    up, down, at = [], [], 0
    pieces = [embed, w_qkv[0], w_qkv[1], w_qkv[2], w_out.T]
    down_t = w_down.T
    for tiles in UP_TILES:
        pieces += [w_up[:, at : at + tiles * TILE], down_t[:, at : at + tiles * TILE]]
        at += tiles * TILE
    whole = gather_weights(jnp.concatenate(pieces, axis=1)).reshape(2, D, COLUMNS)

    def columns(start, size):
        return jnp.concatenate([whole[0, :, start : start + size], whole[1, :, start : start + size]], 1)

    embed_all = columns(0, 512).reshape(64, 16, D)[:, :12].reshape(768, D)
    tokens = jnp.dot(picture, embed_all, preferred_element_type=jnp.float32).astype(jnp.bfloat16)
    normed = layer_norm(tokens.astype(jnp.float32), ln1_gain).astype(jnp.bfloat16)
    q, k, v = (
        jnp.dot(normed, columns(512 * (i + 1), 512), preferred_element_type=jnp.float32)
        for i in range(3)
    )
    q = q * HEAD ** (-0.5)
    q, k, v = (a.astype(jnp.bfloat16).reshape(patches, 16, HEAD).transpose(1, 0, 2) for a in (q, k, v))
    length = counts[0, me]
    usable = jnp.arange(patches, dtype=jnp.int32) < length
    scores = jnp.einsum("hqd,hkd->hqk", q, k, preferred_element_type=jnp.float32)
    scores = jnp.where(usable[None, None, :], scores, -1e30)
    expo = jnp.exp(scores - jnp.max(scores, axis=-1, keepdims=True))
    row_sum = jnp.sum(expo, axis=-1)
    mixed = jnp.einsum("hqk,hkd->hqd", expo.astype(jnp.bfloat16), v, preferred_element_type=jnp.float32)
    attended = (mixed / row_sum[..., None]).astype(jnp.bfloat16).transpose(1, 0, 2).reshape(patches, D)
    residual = tokens.astype(jnp.float32) + jnp.einsum(
        "pk,nk->pn", attended, columns(2048, 512), preferred_element_type=jnp.float32
    )
    normed_two = layer_norm(residual, ln2_gain).astype(jnp.bfloat16)
    output, at = residual, 2560
    for tiles in UP_TILES:
        size = tiles * TILE
        hidden = jax.nn.gelu(
            jnp.dot(normed_two, columns(at, size), preferred_element_type=jnp.float32),
            approximate=False,
        ).astype(jnp.bfloat16)
        output = output + jnp.einsum(
            "pk,nk->pn", hidden, columns(at + size, size), preferred_element_type=jnp.float32
        )
        at += 2 * size
    rows_own = patches // 2
    halves = output.astype(jnp.bfloat16).reshape(2, rows_own, D)
    by_image = lax.all_to_all(halves, "mp", 0, 0, tiled=True)
    by_step = jnp.take(by_image, owner[0], axis=0)
    lengths = jnp.take(counts[0], owner[0])
    row_ids = me * rows_own + jnp.arange(rows_own, dtype=jnp.int32)
    kept = row_ids[None, :] < lengths[:, None]
    misfit = by_step.astype(jnp.float32) - targets[0].astype(jnp.float32)
    squares = jnp.sum(jnp.where(kept[:, :, None], misfit * misfit, 0.0))
    number = jnp.sum(kept.astype(jnp.float32))
    totals = lax.psum(jnp.stack([squares, number]), DP_MP)
    return (by_step[None], totals[0] / (D * totals[1]))


def solution(mesh):
    split = Mesh(mesh.devices.reshape(4, 4, 4, mesh.shape["mp"]), ("dp_0", "dp_1", "dp_2", "mp"))
    return jax.shard_map(
        on_device,
        mesh=split,
        in_specs=(
            P(DP_MP, None, None),
            P(DP, None),
            P(DP, None),
            P(DP, "mp"),
            P(None, DP, "mp"),
            P("mp", DP),
            P(DP, "mp"),
            P("mp", DP),
            P(),
            P(),
            P(DP, None, "mp", None),
        ),
        out_specs=(P(DP, None, "mp", None), P()),
        check_vma=False,
    )
```

```python
import jax
import jax.numpy as jnp
from jax import lax
from jax.experimental import pallas as pl
from jax.experimental.pallas import tpu as pltpu
from jax.sharding import Mesh
from jax.sharding import PartitionSpec as P

D = 1024
HEAD = 64
DP = ("dp_0", "dp_1", "dp_2")
DP_MP = ("dp_0", "dp_1", "dp_2", "mp")
MESH = pl.DeviceIdType.MESH
TILE = 128
ORDERS = ((2, 1, 0), (1, 0, 2), (0, 2, 1))
BATCHES = ((6, 5, 5), (4, 4, 4), (4, 4, 4), (4, 4, 4))
UP_TILES = (4, 6, 6)
COLUMNS = TILE * sum(sum(b) for b in BATCHES)


def spans():
    out, at = [], 0
    for batch in BATCHES:
        row = []
        for tiles in batch:
            row.append((at * TILE, tiles * TILE))
            at += tiles
        out.append(row)
    return out


SPANS = spans()


class Gather:

    def __init__(self, whole_ref, send_sems, recv_sems):
        self.whole = whole_ref
        self.send, self.recv = send_sems, recv_sems
        self.me = [lax.axis_index(a) for a in DP]
        self.half = lax.axis_index("mp")
        self.copies = {}
        self.count = 0
        self.started = []

    def region(self, order, phase, coord, start, size):
        at = [None, None, None]
        for i in range(3):
            axis = order[i]
            at[axis] = pl.ds(0, 4) if i < phase else (coord if i == phase else self.me[axis])
        return self.whole.at[self.half, at[0], at[1], at[2], :, pl.ds(start, size)]

    def copy(self, key, src, dst, device):
        made = pltpu.make_async_remote_copy(
            src_ref=src,
            dst_ref=dst,
            send_sem=self.send.at[self.count],
            recv_sem=self.recv.at[self.count],
            device_id=device,
            device_id_type=MESH,
        )
        self.count += 1
        made.start()
        self.started.append(made)
        self.copies[key] = made

    def ring(self, batch, colour, phase):
        order = ORDERS[colour]
        axis = order[phase]
        mine = self.me[axis]
        right, left = lax.rem(mine + 1, 4), lax.rem(mine + 3, 4)
        return order, DP[axis], mine, right, left

    def step_a(self, batch, phase):
        for colour in range(3):
            if phase > 0:
                for side in "rl":
                    self.copies[batch, colour, phase - 1, "b", side].wait_recv()
            order, name, mine, right, left = self.ring(batch, colour, phase)
            start, size = SPANS[batch][colour]
            block = self.region(order, phase, mine, start, size)
            self.copy((batch, colour, phase, "a", "r"), block, block, {name: right})
            self.copy((batch, colour, phase, "a", "l"), block, block, {name: left})
            if phase == 2:
                self.across(batch, colour, mine)

    def step_b(self, batch, phase):
        for colour in range(3):
            for side in "rl":
                self.copies[batch, colour, phase, "a", side].wait_recv()
            order, name, mine, right, left = self.ring(batch, colour, phase)
            start, size = SPANS[batch][colour]
            first = size // TILE // 2 * TILE
            from_left = self.region(order, phase, left, start, first)
            from_right = self.region(order, phase, right, start + first, size - first)
            self.copy((batch, colour, phase, "b", "r"), from_left, from_left, {name: right})
            self.copy((batch, colour, phase, "b", "l"), from_right, from_right, {name: left})
            if phase == 2:
                self.across(batch, colour, left)
                self.across(batch, colour, right)

    def across(self, batch, colour, coord):
        start, size = SPANS[batch][colour]
        block = self.region(ORDERS[colour], 2, coord, start, size)
        kind = sum(1 for k in self.copies if k[:2] == (batch, colour) and k[2] == "x")
        self.copy((batch, colour, "x", kind), block, block, {"mp": 1 - self.half})

    def finish(self, batch):
        for colour in range(3):
            for side in "rl":
                self.copies[batch, colour, 2, "b", side].wait_recv()
            mine = self.me[ORDERS[colour][2]]
            self.across(batch, colour, lax.rem(mine + 2, 4))

    def arrived(self, batch):
        for colour in range(3):
            for kind in range(4):
                self.copies[batch, colour, "x", kind].wait_recv()

    def drain(self):
        for made in self.started:
            made.wait_send()


def greet():
    barrier = pltpu.get_barrier_semaphore()
    count = 0
    for name in DP:
        mine = lax.axis_index(name)
        for step in (1, 2, 3):
            pl.semaphore_signal(
                barrier, inc=1, device_id={name: lax.rem(mine + step, 4)}, device_id_type=MESH
            )
            count += 1
    pl.semaphore_signal(
        barrier, inc=1, device_id={"mp": 1 - lax.axis_index("mp")}, device_id_type=MESH
    )
    pl.semaphore_wait(barrier, count + 1)


def layer_norm(inputs, gains):
    average = jnp.mean(inputs, axis=-1, keepdims=True)
    centred = inputs - average
    spread = jnp.mean(centred * centred, axis=-1, keepdims=True)
    return centred * lax.rsqrt(spread + 1e-06) * gains


def dot(a, b):
    return jnp.dot(a, b, preferred_element_type=jnp.float32)


def dot_t(a, b):
    return lax.dot_general(a, b, (((1,), (1,)), ((), ())), preferred_element_type=jnp.float32)


BF = jnp.bfloat16
N_COPIES = len(BATCHES) * 3 * 16
ROWS = 512
OWN = 256


def encode_kernel(
    counts,
    owner,
    picture,
    embed,
    w_qkv,
    w_out,
    w_up,
    w_down,
    gain1,
    gain2,
    targets,
    encoded,
    loss,
    whole,
    spread,
    tokens,
    normed,
    queries,
    key_rows,
    value_rows,
    attended,
    total,
    sending,
    by_image,
    sums,
    send_sems,
    recv_sems,
    end_send,
    end_recv,
):
    half = lax.axis_index("mp")
    me = [lax.axis_index(a) for a in DP]
    eye = (
        lax.broadcasted_iota(jnp.int32, (16, 16), 0) == lax.broadcasted_iota(jnp.int32, (16, 16), 1)
    ).astype(BF)

    def place(start, value):
        whole[half, me[0], me[1], me[2], :, pl.ds(start, value.shape[1])] = value

    place(0, jnp.concatenate([embed[...].astype(jnp.float32), jnp.zeros((4, 512), jnp.float32)], 0).astype(BF))
    for i in range(3):
        place(512 * (i + 1), w_qkv[i])
    place(2048, dot_t(eye, w_out[...]).astype(BF))
    at, hidden_at = 2560, 0
    for tiles in UP_TILES:
        size = tiles * TILE
        place(at, w_up[:, pl.ds(hidden_at, size)])
        place(at + size, dot_t(eye, w_down[pl.ds(hidden_at, size), :]).astype(BF))
        at += 2 * size
        hidden_at += size
    greet()
    g = Gather(whole, send_sems, recv_sems)

    def weights(h, start, size):
        return whole[h, :, :, :, :, pl.ds(start, size)].reshape(D, size)

    for b in range(4):
        g.step_a(b, 0)
    from_px = lax.broadcasted_iota(jnp.int32, (768, D), 0)
    column = lax.broadcasted_iota(jnp.int32, (768, D), 1)
    within = lax.bitwise_and(column, 15)
    to_px = lax.shift_right_logical(column, 4) * 12 + within
    pick = jnp.where((from_px == to_px) & (within < 12), 1.0, 0.0).astype(BF)
    spread[...] = dot(picture[...], pick).astype(BF)
    for b in range(4):
        g.step_b(b, 0)
    g.step_a(0, 1)
    g.step_a(1, 1)
    g.step_b(0, 1)
    g.step_a(0, 2)
    g.step_b(1, 1)
    g.step_a(2, 1)
    g.step_b(0, 2)
    g.step_b(2, 1)
    g.step_a(1, 2)
    g.step_a(3, 1)
    g.finish(0)
    g.arrived(0)
    for h in range(2):
        tokens[:, pl.ds(512 * h, 512)] = dot(spread[...], weights(h, 0, 512)).astype(BF)
    normed[...] = layer_norm(tokens[...].astype(jnp.float32), gain1[...]).astype(BF)
    g.step_b(1, 2)
    g.step_b(3, 1)
    g.step_a(2, 2)
    for i, (ref, factor) in enumerate(((queries, HEAD ** (-0.5)), (key_rows, 1.0), (value_rows, 1.0))):
        for h in range(2):
            part = dot(normed[...], weights(h, 512 * (i + 1), 512))
            if factor != 1.0:
                part = part * factor
            part = part.astype(BF)
            for j in range(4):
                ref[4 * h + j] = part[:, 128 * j : 128 * (j + 1)]
    g.finish(1)
    length = counts[0, half]
    key_id = lax.broadcasted_iota(jnp.int32, (1, ROWS), 1)
    bias = jnp.where(key_id < length, 0.0, -1e30)
    low = lax.broadcasted_iota(jnp.int32, (ROWS, 128), 1) < HEAD

    def pair(i, carry):
        q, k, v = queries[i], key_rows[i], value_rows[i]
        none, one = jnp.zeros_like(q), jnp.ones_like(v)

        def head(q_part, v_part):
            scores = dot_t(q_part, k) + bias
            expo = jnp.exp(scores - jnp.max(scores, axis=-1, keepdims=True))
            return dot(expo.astype(BF), v_part)

        first = head(jnp.where(low, q, none), jnp.where(low, v, one))
        second = head(jnp.where(low, none, q), jnp.where(low, one, v))
        values = jnp.where(low, first, second)
        row_sums = pltpu.roll(jnp.where(low, second, first), HEAD, 1)
        attended[i] = (values / row_sums).astype(BF)
        return carry

    lax.fori_loop(0, 3, pair, 0)
    g.step_b(2, 2)
    g.step_a(3, 2)
    lax.fori_loop(3, 8, pair, 0)
    g.finish(2)
    residual = tokens[...].astype(jnp.float32)
    g.arrived(1)
    for h in range(2):
        mixed = jnp.concatenate([attended[4 * h + j] for j in range(4)], axis=1)
        residual = residual + dot_t(mixed, weights(h, 2048, 512))
    total[...] = residual
    normed[...] = layer_norm(residual, gain2[...]).astype(BF)
    g.step_b(3, 2)

    def mlp(rows, h, at, size):
        hidden = dot(normed[rows, :], weights(h, at, size))
        hidden = hidden * 0.5 * (1.0 + lax.erf(hidden * (0.5**0.5)))
        return dot_t(hidden.astype(BF), weights(h, at + size, size))

    everything = pl.ds(0, ROWS)
    total[...] += mlp(everything, 0, 2560, 512)
    total[...] += mlp(everything, 1, 2560, 512)
    g.finish(3)
    g.arrived(2)
    total[...] += mlp(everything, 0, 3584, 768)
    total[...] += mlp(everything, 1, 3584, 768)
    g.arrived(3)
    other = 1 - half
    for piece, mine in ((other, False), (half, True)):
        rows = pl.ds(pl.multiple_of(piece * OWN, OWN), OWN)
        result = (total[rows, :] + mlp(rows, 0, 5120, 768) + mlp(rows, 1, 5120, 768)).astype(BF)
        if mine:
            by_image[half] = result
        else:
            sending[...] = result
            exchange = pltpu.make_async_remote_copy(
                src_ref=sending,
                dst_ref=by_image.at[half],
                send_sem=end_send.at[0],
                recv_sem=end_recv.at[0],
                device_id={"mp": other},
                device_id_type=MESH,
            )
            exchange.start()
    exchange.wait_recv()
    row_id = half * OWN + lax.broadcasted_iota(jnp.int32, (OWN, 1), 0)
    squares = jnp.zeros((8, 128), jnp.float32)
    number = jnp.zeros((8, 128), jnp.float32)
    for step in range(2):
        source = owner[0, step]
        valid = jnp.where(source == 0, counts[0, 0], counts[0, 1])
        rows = jnp.where(source == 0, by_image[0].astype(jnp.float32), by_image[1].astype(jnp.float32))
        encoded[step] = rows.astype(BF)
        misfit = rows - targets[step].astype(jnp.float32)
        misfit = jnp.where(row_id < valid, misfit * misfit, 0.0)
        squares = squares + misfit.reshape(OWN // 8, 8, 8, 128).sum(axis=(0, 2))
        number = number + jnp.clip(valid - half * OWN, 0, OWN).astype(jnp.float32)
    both = jnp.concatenate([squares, number], 0)
    at = 1
    lines = [("mp", 2, half)] + [(name, 4, mine) for name, mine in zip(DP, me)]
    for stage, (name, members, mine) in enumerate(lines):
        sums[stage, mine] = both
        sent = []
        for step in range(1, members):
            made = pltpu.make_async_remote_copy(
                src_ref=sums.at[stage, mine],
                dst_ref=sums.at[stage, mine],
                send_sem=end_send.at[at],
                recv_sem=end_recv.at[at],
                device_id={name: lax.rem(mine + step, members)},
                device_id_type=MESH,
            )
            made.start()
            sent.append(made)
            at += 1
        for made in sent:
            made.wait_recv()
        both = sums[stage, 0]
        for other_member in range(1, members):
            both = both + sums[stage, other_member]
        for made in sent:
            made.wait_send()
    mean = jnp.sum(both[:8]) / (D * jnp.max(both[8:]))
    loss[...] = jnp.full((8, 128), mean, jnp.float32)
    exchange.wait_send()
    g.drain()


def on_device(
    pixels, counts, owner, embed_weight, w_qkv, w_out, w_up, w_down, ln1_gain, ln2_gain, targets
):
    vmem = pl.BlockSpec(memory_space=pltpu.VMEM)
    smem = pl.BlockSpec(memory_space=pltpu.SMEM)
    encoded, loss = pl.pallas_call(
        encode_kernel,
        out_shape=(
            jax.ShapeDtypeStruct((2, OWN, D), BF),
            jax.ShapeDtypeStruct((8, 128), jnp.float32),
        ),
        in_specs=[smem, smem] + [vmem] * 9,
        out_specs=(vmem, vmem),
        scratch_shapes=[
            pltpu.VMEM((2, 4, 4, 4, 16, COLUMNS), BF),
            pltpu.VMEM((ROWS, D), BF),
            pltpu.VMEM((ROWS, D), BF),
            pltpu.VMEM((ROWS, D), BF),
            pltpu.VMEM((8, ROWS, 128), BF),
            pltpu.VMEM((8, ROWS, 128), BF),
            pltpu.VMEM((8, ROWS, 128), BF),
            pltpu.VMEM((8, ROWS, 128), BF),
            pltpu.VMEM((ROWS, D), jnp.float32),
            pltpu.VMEM((OWN, D), BF),
            pltpu.VMEM((2, OWN, D), BF),
            pltpu.VMEM((4, 4, 16, 128), jnp.float32),
            pltpu.SemaphoreType.DMA((N_COPIES,)),
            pltpu.SemaphoreType.DMA((N_COPIES,)),
            pltpu.SemaphoreType.DMA((11,)),
            pltpu.SemaphoreType.DMA((11,)),
        ],
        compiler_params=pltpu.CompilerParams(
            collective_id=0, has_side_effects=True, vmem_limit_bytes=64 * 1024 * 1024 - 65536
        ),
        name="encode",
    )(
        counts,
        owner,
        pixels[0],
        embed_weight,
        w_qkv,
        w_out,
        w_up,
        w_down,
        ln1_gain[None],
        ln2_gain[None],
        targets[0],
    )
    return (encoded[None], loss[0, 0])


def solution(mesh):
    split = Mesh(mesh.devices.reshape(4, 4, 4, mesh.shape["mp"]), ("dp_0", "dp_1", "dp_2", "mp"))
    return jax.shard_map(
        on_device,
        mesh=split,
        in_specs=(
            P(DP_MP, None, None),
            P(DP, None),
            P(DP, None),
            P(DP, "mp"),
            P(None, DP, "mp"),
            P("mp", DP),
            P(DP, "mp"),
            P("mp", DP),
            P(),
            P(),
            P(DP, None, "mp", None),
        ),
        out_specs=(P(DP, None, "mp", None), P()),
        check_vma=False,
    )
```

```python
import jax
import jax.numpy as jnp
from jax import lax
from jax.experimental import pallas as pl
from jax.experimental.pallas import tpu as pltpu
from jax.sharding import Mesh
from jax.sharding import PartitionSpec as P

D = 1024
HEAD = 64
ROWS = 512
OWN = 256
DP = ("dp_0", "dp_1", "dp_2")
DP_MP = ("dp_0", "dp_1", "dp_2", "mp")
MESH = pl.DeviceIdType.MESH
BF = jnp.bfloat16
TILE = 128
ORDERS = ((2, 1, 0), (1, 0, 2), (0, 2, 1))
BATCHES = ((2, 2, 2), (3, 2, 2), (2, 3, 2), (3, 2, 3), (2, 3, 3), (3, 3, 2), (2, 3, 3))
COUNT = len(BATCHES)
TILES = sum(sum(b) for b in BATCHES)
COLUMNS = TILE * TILES


def place_tiles():
    base = [sum(b[c] for b in BATCHES) for c in range(3)]
    base = [0, base[0], base[0] + base[1]]
    where, spans = [], []
    at = list(base)
    for batch in BATCHES:
        spans.append([at[c] for c in range(3)])
        for c in range(3):
            where += list(range(at[c], at[c] + batch[c]))
            at[c] += batch[c]
    spans.append(at)
    return where, spans


WHERE, SPANS = place_tiles()


def runs(first, tiles):
    found = []
    for t in range(first, first + tiles):
        if found and found[-1][0] + found[-1][1] == WHERE[t]:
            found[-1][1] += 1
        else:
            found.append([WHERE[t], 1])
    return [(a * TILE, n * TILE) for a, n in found]


class Gather:

    def __init__(self, whole, send_sems, recv_sems):
        self.whole, self.send, self.recv = whole, send_sems, recv_sems
        self.me = [lax.axis_index(a) for a in DP]
        self.half = lax.axis_index("mp")
        self.sems = {}
        self.done = set()

    def span(self, group, colour):
        start = SPANS[group[0]][colour] * TILE
        return start, SPANS[group[1]][colour] * TILE - start

    def region(self, colour, phase, coord, start, size):
        at = [None, None, None]
        for i, axis in enumerate(ORDERS[colour]):
            at[axis] = pl.ds(0, 4) if i < phase else (coord if i == phase else self.me[axis])
        return self.whole.at[self.half, at[0], at[1], at[2], :, pl.ds(start, size)]

    def sem(self, key):
        return self.sems.setdefault(key, len(self.sems))

    def copy(self, key, block, device):
        at = self.sem(key)
        pltpu.make_async_remote_copy(
            src_ref=block,
            dst_ref=block,
            send_sem=self.send.at[at],
            recv_sem=self.recv.at[at],
            device_id=device,
            device_id_type=MESH,
        ).start()

    def all_of(self, key):
        group, phase, step = key
        size = sum(self.span(group, c)[1] for c in range(3))
        slots = {"x": 64, "a": 2 * 4 ** phase, "b": 4 ** phase, "d": 3 * 4 ** phase}[step]
        z, y, x = max(slots // 16, 1), min(max(slots // 4, 1), 4), min(slots, 4)
        assert z * y * x == slots
        block = self.whole.at[self.half, pl.ds(0, z), pl.ds(0, y), pl.ds(0, x), :, pl.ds(0, size)]
        at = self.sem(key)
        return pltpu.make_async_remote_copy(
            src_ref=block,
            dst_ref=block,
            send_sem=self.send.at[at],
            recv_sem=self.recv.at[at],
            device_id={"mp": 1 - self.half},
            device_id_type=MESH,
        )

    def wait(self, group, phase, step):
        self.all_of((group, phase, step)).wait_recv()

    def line(self, colour, phase):
        axis = ORDERS[colour][phase]
        mine = self.me[axis]
        return DP[axis], mine, lax.rem(mine + 1, 4), lax.rem(mine + 3, 4)

    def a(self, group, phase):
        for colour in range(3):
            name, mine, right, left = self.line(colour, phase)
            block = self.region(colour, phase, mine, *self.span(group, colour))
            self.copy((group, phase, "a"), block, {name: right})
            self.copy((group, phase, "a"), block, {name: left})
        if phase == 2:
            self.across(group, 0)

    def d(self, group, phase):
        for colour in range(3):
            name, mine, _, _ = self.line(colour, phase)
            block = self.region(colour, phase, mine, *self.span(group, colour))
            for step in (1, 3, 2):
                self.copy((group, phase, "d"), block, {name: lax.rem(mine + step, 4)})

    def b(self, group, phase):
        self.wait(group, phase, "a")
        for colour in range(3):
            name, mine, right, left = self.line(colour, phase)
            start, size = self.span(group, colour)
            first = (size // TILE + colour % 2) // 2 * TILE
            from_left = self.region(colour, phase, left, start, first)
            from_right = self.region(colour, phase, right, start + first, size - first)
            self.copy((group, phase, "b"), from_left, {name: right})
            self.copy((group, phase, "b"), from_right, {name: left})
        if phase == 2:
            self.across(group, 1)
            self.across(group, 3)

    def across(self, group, step):
        for colour in range(3):
            coord = lax.rem(self.me[ORDERS[colour][2]] + step, 4)
            block = self.region(colour, 2, coord, *self.span(group, colour))
            self.copy((group, 2, "x"), block, {"mp": 1 - self.half})

    def finish(self, group):
        self.wait(group, 2, "b")
        self.across(group, 2)

    def arrived(self, group):
        self.wait(group, 2, "x")

    def drain(self):
        for key in self.sems:
            self.all_of(key).wait_send()


def layer_norm(inputs, gains):
    average = jnp.mean(inputs, axis=-1, keepdims=True)
    centred = inputs - average
    spread = jnp.mean(centred * centred, axis=-1, keepdims=True)
    return centred * lax.rsqrt(spread + 1e-06) * gains


def dot(a, b):
    return jnp.dot(a, b, preferred_element_type=jnp.float32)


def dot_t(a, b):
    return lax.dot_general(a, b, (((1,), (1,)), ((), ())), preferred_element_type=jnp.float32)


def encode_kernel(
    counts,
    owner,
    pixels,
    embed,
    w_qkv,
    w_out,
    w_up,
    w_down,
    gain1,
    gain2,
    aims,
    encoded,
    loss,
    whole,
    picture,
    targets,
    outcome,
    spread,
    tokens,
    normed,
    queries,
    key_rows,
    value_rows,
    attended,
    total,
    sending,
    by_image,
    sums,
    send_sems,
    recv_sems,
    end_send,
    end_recv,
    local_sems,
):
    half = lax.axis_index("mp")
    other = 1 - half
    me = [lax.axis_index(a) for a in DP]
    get_picture = pltpu.make_async_copy(pixels, picture, local_sems.at[0])
    get_targets = pltpu.make_async_copy(aims, targets, local_sems.at[1])
    get_picture.start()
    get_targets.start()
    barrier = pltpu.get_barrier_semaphore()
    for name, mine in zip(DP, me):
        for step in (1, 2, 3):
            pl.semaphore_signal(
                barrier, inc=1, device_id={name: lax.rem(mine + step, 4)}, device_id_type=MESH
            )
    pl.semaphore_signal(barrier, inc=1, device_id={"mp": other}, device_id_type=MESH)

    def place(first, value):
        at = 0
        for start, size in runs(first, value.shape[1] // TILE):
            whole[half, me[0], me[1], me[2], :, pl.ds(start, size)] = value[:, at : at + size]
            at += size

    padded = [embed[...].astype(jnp.float32), jnp.zeros((4, 512), jnp.float32)]
    place(0, jnp.concatenate(padded, 0).astype(BF))
    for i in range(3):
        place(4 + 4 * i, w_qkv[i])
    place(16, w_out[...])
    for i in range(4):
        place(20 + 8 * i, w_up[:, pl.ds(512 * i, 512)])
        place(24 + 8 * i, w_down[:, pl.ds(512 * i, 512)])
    from_px = lax.broadcasted_iota(jnp.int32, (768, D), 0)
    column = lax.broadcasted_iota(jnp.int32, (768, D), 1)
    within = lax.bitwise_and(column, 15)
    to_px = lax.shift_right_logical(column, 4) * 12 + within
    pick = jnp.where((from_px == to_px) & (within < 12), 1.0, 0.0).astype(BF)
    pl.semaphore_wait(barrier, 10)
    g = Gather(whole, send_sems, recv_sems)

    def weights(h, first, tiles):
        parts = [whole[h, :, :, :, :, pl.ds(a, n)].reshape(D, n) for a, n in runs(first, tiles)]
        return parts[0] if len(parts) == 1 else jnp.concatenate(parts, axis=1)

    one = [(i, i + 1) for i in range(COUNT)]
    head, tail, second, third, fourth = (0, 3), (3, 7), (1, 3), (3, 5), (5, 7)
    g.d(head, 0)
    g.a(tail, 0)
    get_picture.wait()
    spread[...] = dot(picture[...], pick).astype(BF)
    g.wait(head, 0, "d")
    g.d(one[0], 1)
    g.a(second, 1)
    g.b(tail, 0)
    g.wait(one[0], 1, "d")
    g.a(one[0], 2)
    g.b(second, 1)
    g.wait(tail, 0, "b")
    g.a(third, 1)
    g.b(one[0], 2)
    g.wait(second, 1, "b")
    g.a(one[1], 2)
    g.a(one[2], 2)
    g.b(third, 1)
    g.a(fourth, 1)
    g.finish(one[0])
    g.b(one[1], 2)
    g.wait(third, 1, "b")
    g.a(one[3], 2)
    g.arrived(one[0])
    for h in range(2):
        tokens[:, pl.ds(512 * h, 512)] = dot(spread[...], weights(h, 0, 4)).astype(BF)
    normed[...] = layer_norm(tokens[...].astype(jnp.float32), gain1[...]).astype(BF)
    g.b(one[2], 2)
    g.b(fourth, 1)
    g.a(one[4], 2)
    g.finish(one[1])

    def project(ref, first, factor):
        for h in range(2):
            part = dot(normed[...], weights(h, first, 4))
            if factor != 1.0:
                part = part * factor
            part = part.astype(BF)
            for j in range(4):
                ref[4 * h + j] = part[:, 128 * j : 128 * (j + 1)]

    g.arrived(one[1])
    project(queries, 4, HEAD ** (-0.5))
    project(key_rows, 8, 1.0)
    g.finish(one[2])
    g.b(one[3], 2)
    g.wait(fourth, 1, "b")
    g.a(one[5], 2)
    g.arrived(one[2])
    project(value_rows, 12, 1.0)
    length = counts[0, half]
    key_id = lax.broadcasted_iota(jnp.int32, (1, ROWS), 1)
    bias = jnp.where(key_id < length, 0.0, -1e30)
    low = lax.broadcasted_iota(jnp.int32, (ROWS, 128), 1) < HEAD

    def pair(i, carry):
        q, k, v = queries[i], key_rows[i], value_rows[i]
        none, ones = jnp.zeros_like(q), jnp.ones_like(v)

        def head_of(q_part, v_part):
            scores = dot_t(q_part, k) + bias
            expo = jnp.exp(scores - jnp.max(scores, axis=-1, keepdims=True))
            return dot(expo.astype(BF), v_part)

        first = head_of(jnp.where(low, q, none), jnp.where(low, v, ones))
        second = head_of(jnp.where(low, none, q), jnp.where(low, ones, v))
        values = jnp.where(low, first, second)
        row_sums = pltpu.roll(jnp.where(low, second, first), HEAD, 1)
        attended[i] = (values / row_sums).astype(BF)
        return carry

    lax.fori_loop(0, 2, pair, 0)
    g.finish(one[3])
    g.b(one[4], 2)
    g.a(one[6], 2)
    lax.fori_loop(2, 5, pair, 0)
    g.finish(one[4])
    g.b(one[5], 2)
    lax.fori_loop(5, 8, pair, 0)
    g.finish(one[5])
    residual = tokens[...].astype(jnp.float32)
    for h in range(2):
        mixed = jnp.concatenate([attended[4 * h + j] for j in range(4)], axis=1)
        residual = residual + dot_t(mixed, weights(h, 16, 4))
    total[...] = residual
    normed[...] = layer_norm(residual, gain2[...]).astype(BF)

    def mlp(rows, quarter):
        found = None
        for h in range(2):
            hidden = dot(normed[rows, :], weights(h, 20 + 8 * quarter, 4))
            hidden = hidden * 0.5 * (1.0 + lax.erf(hidden * (0.5**0.5)))
            part = dot_t(hidden.astype(BF), weights(h, 24 + 8 * quarter, 4))
            found = part if found is None else found + part
        return found

    everything = pl.ds(0, ROWS)
    g.b(one[6], 2)
    g.arrived(one[3])
    total[...] += mlp(everything, 0)
    g.arrived(one[4])
    total[...] += mlp(everything, 1)
    g.finish(one[6])
    g.arrived(one[5])
    total[...] += mlp(everything, 2)
    g.arrived(one[6])
    for piece, mine in ((other, False), (half, True)):
        rows = pl.ds(pl.multiple_of(piece * OWN, OWN), OWN)
        result = (total[rows, :] + mlp(rows, 3)).astype(BF)
        if mine:
            by_image[half] = result
        else:
            sending[...] = result
            exchange = pltpu.make_async_remote_copy(
                src_ref=sending,
                dst_ref=by_image.at[half],
                send_sem=end_send.at[0],
                recv_sem=end_recv.at[0],
                device_id={"mp": other},
                device_id_type=MESH,
            )
            exchange.start()
    get_targets.wait()
    exchange.wait_recv()
    row_id = half * OWN + lax.broadcasted_iota(jnp.int32, (OWN, 1), 0)
    squares = jnp.zeros((8, 128), jnp.float32)
    number = jnp.zeros((8, 128), jnp.float32)
    for step in range(2):
        source = owner[0, step]
        valid = jnp.where(source == 0, counts[0, 0], counts[0, 1])
        rows = jnp.where(source == 0, by_image[0].astype(jnp.float32), by_image[1].astype(jnp.float32))
        outcome[step] = rows.astype(BF)
        misfit = rows - targets[step].astype(jnp.float32)
        misfit = jnp.where(row_id < valid, misfit * misfit, 0.0)
        squares = squares + misfit.reshape(OWN // 8, 8, 8, 128).sum(axis=(0, 2))
        number = number + jnp.clip(valid - half * OWN, 0, OWN).astype(jnp.float32)
    both = jnp.concatenate([squares, number], 0)
    at = 1
    lines = [("mp", 2, half)] + [(name, 4, mine) for name, mine in zip(DP, me)]
    for stage, (name, members, mine) in enumerate(lines):
        sums[stage, mine] = both
        sent = []
        for step in range(1, members):
            made = pltpu.make_async_remote_copy(
                src_ref=sums.at[stage, mine],
                dst_ref=sums.at[stage, mine],
                send_sem=end_send.at[at],
                recv_sem=end_recv.at[at],
                device_id={name: lax.rem(mine + step, members)},
                device_id_type=MESH,
            )
            made.start()
            sent.append(made)
            at += 1
        if stage == 0:
            put = pltpu.make_async_copy(outcome, encoded, local_sems.at[2])
            put.start()
            g.drain()
            exchange.wait_send()
        for made in sent:
            made.wait_recv()
        both = sums[stage, 0]
        for member in range(1, members):
            both = both + sums[stage, member]
        for made in sent:
            made.wait_send()
    mean = jnp.sum(both[:8]) / (D * jnp.max(both[8:]))
    loss[...] = jnp.full((1, 1), mean, jnp.float32)
    put.wait()


N_SEMS = 40


def on_device(
    pixels, counts, owner, embed_weight, w_qkv, w_out, w_up, w_down, ln1_gain, ln2_gain, targets
):
    vmem = pl.BlockSpec(memory_space=pltpu.VMEM)
    smem = pl.BlockSpec(memory_space=pltpu.SMEM)
    hbm = pl.BlockSpec(memory_space=pl.ANY)
    encoded, loss = pl.pallas_call(
        encode_kernel,
        out_shape=(
            jax.ShapeDtypeStruct((2, OWN, D), BF),
            jax.ShapeDtypeStruct((1, 1), jnp.float32),
        ),
        in_specs=[smem, smem, hbm] + [vmem] * 7 + [hbm],
        out_specs=(hbm, vmem),
        scratch_shapes=[
            pltpu.VMEM((2, 4, 4, 4, 16, COLUMNS), BF),
            pltpu.VMEM((ROWS, 768), BF),
            pltpu.VMEM((2, OWN, D), BF),
            pltpu.VMEM((2, OWN, D), BF),
            pltpu.VMEM((ROWS, D), BF),
            pltpu.VMEM((ROWS, D), BF),
            pltpu.VMEM((ROWS, D), BF),
            pltpu.VMEM((8, ROWS, 128), BF),
            pltpu.VMEM((8, ROWS, 128), BF),
            pltpu.VMEM((8, ROWS, 128), BF),
            pltpu.VMEM((8, ROWS, 128), BF),
            pltpu.VMEM((ROWS, D), jnp.float32),
            pltpu.VMEM((OWN, D), BF),
            pltpu.VMEM((2, OWN, D), BF),
            pltpu.VMEM((4, 4, 16, 128), jnp.float32),
            pltpu.SemaphoreType.DMA((N_SEMS,)),
            pltpu.SemaphoreType.DMA((N_SEMS,)),
            pltpu.SemaphoreType.DMA((11,)),
            pltpu.SemaphoreType.DMA((11,)),
            pltpu.SemaphoreType.DMA((3,)),
        ],
        compiler_params=pltpu.CompilerParams(
            collective_id=0, has_side_effects=True, vmem_limit_bytes=64 * 1024 * 1024 - 65536
        ),
        name="encode",
    )(
        counts,
        owner,
        pixels[0],
        embed_weight,
        w_qkv,
        w_out.T,
        w_up,
        w_down.T,
        ln1_gain[None],
        ln2_gain[None],
        targets[0],
    )
    return (encoded[None], loss[0, 0])


def solution(mesh):
    split = Mesh(mesh.devices.reshape(4, 4, 4, mesh.shape["mp"]), ("dp_0", "dp_1", "dp_2", "mp"))
    return jax.shard_map(
        on_device,
        mesh=split,
        in_specs=(
            P(DP_MP, None, None),
            P(DP, None),
            P(DP, None),
            P(DP, "mp"),
            P(None, DP, "mp"),
            P("mp", DP),
            P(DP, "mp"),
            P("mp", DP),
            P(),
            P(),
            P(DP, None, "mp", None),
        ),
        out_specs=(P(DP, None, "mp", None), P()),
        check_vma=False,
    )
```
